128 devices in a mesh: gx: 8 (over x, core), gy: 16 (over z, y).
Axes of the slice: x: 4, y: 4, z: 4, core: 2. Of those that a mesh axis runs over, the one named last changes fastest.
Arguments:
- mask_feats: bfloat16 [256, 8, 14, 14, 256], P(('gx', 'gy')), may hold values from -6 to 6
- mask_cot: bfloat16 [256, 8, 14, 14, 256], P(('gx', 'gy')), may hold values from -6 to 6
- roi_counts: int32 [256], P(('gx', 'gy')), may hold values from 1 to 8, as said below
- rpn_feats: bfloat16 [256, 48, 32, 256], P(('gx', 'gy')), may hold values from -6 to 6
- rpn_cot: bfloat16 [256, 48, 32, 256], P(('gx', 'gy')), may hold values from -360 to 360
- anchor_counts: int32 [256], P(('gx', 'gy')), may hold values from 32 to 223
- mask_weight: float32 [2304, 256], replicated, may hold values from -0.125 to 0.125
- rpn_weight: float32 [2304, 256], replicated, may hold values from -0.125 to 0.125
- mask_moment: float32 [2304, 256], replicated, may hold values from -6 to 6
- rpn_moment: float32 [2304, 256], replicated, may hold values from -6 to 6
Outputs:
- new_mask_weight: float32 [2304, 256], replicated
- new_rpn_weight: float32 [2304, 256], replicated
- new_mask_moment: float32 [2304, 256], replicated
- new_rpn_moment: float32 [2304, 256], replicated
The draws below stay inside these ranges and needn't reach their ends.
Inputs may be any that keep to these rules, and one draw needn't show every extreme that they name: `roi_counts`: every image has at least one positive ROI; some image has all 8 slots positive.
All inputs are finite; a program needn't handle non-finite values.
Results may differ from the reference program's by a relative error of at most 0.0003.
Values sent between devices are 32-bit elements; how exact they have to be, the bound alone decides.
A program may use at most 128 MiB of HBM per device.

```python
import jax
import jax.numpy as jnp
from jax import lax

C = 256
MH = 14
ROI_IMG = 8
IMG_DEV = 2
GH = 48
GW = 32
IMAGES = 256
N_GX = 8
N_GY = 16


def rising_level():
    image = jnp.arange(IMAGES, dtype=jnp.int32)
    device = image // IMG_DEV
    x_index = device // N_GY
    y_index = device % N_GY
    x_span = max(N_GX - 1, 1)
    y_span = max(N_GY - 1, 1)
    numer = x_index * y_span + y_index * x_span
    denom = 2 * x_span * y_span
    return (image, numer, denom)


def draw_roi_counts(key, part):
    image, numer, denom = rising_level()
    lowest = 1 + ROI_IMG * 5 // 8 * numer // denom
    extra = jax.random.randint(jax.random.fold_in(key, 11), (IMAGES,), 0, 3)
    counts = jnp.minimum(lowest + extra, ROI_IMG)
    counts = jnp.where(image == IMAGES - 1, ROI_IMG, counts)
    return counts.astype(jnp.int32)


def draw_anchor_counts(key, part):
    image, numer, denom = rising_level()
    lowest = 32 + 96 * numer // denom
    extra = jax.random.randint(jax.random.fold_in(key, 23), (IMAGES,), 0, 96)
    return (lowest + extra).astype(jnp.int32)


def level_of(own_key, shape, cuts, least, largest):
    gain = 1.0
    for axis_at, shards_of in cuts:
        draws = jax.random.uniform(jax.random.fold_in(jax.random.fold_in(own_key, 6), axis_at), (shards_of,), jnp.float32, least / len(cuts), largest / len(cuts))
        gain = gain * jnp.repeat(jnp.exp(draws), shape[axis_at] // shards_of).reshape((-1,) + (1,) * (len(shape) - 1 - axis_at))
    return gain


def bell_draw(key, shape, spread, limit, pieces=(), held_as=jnp.bfloat16):
    loudness = level_of(key, shape, pieces, -0.22, 0.18) if pieces else 1.0
    result = jax.random.normal(key, shape, jnp.float32) * spread * loudness
    return jnp.minimum(jnp.maximum(result, -limit), limit).astype(held_as)


def setup_inputs(seed: int = 0) -> dict:
    key_list = jax.random.split(jax.random.key(seed), 11)
    return {
        "mask_feats": bell_draw(key_list[0], (IMAGES, ROI_IMG, MH, MH, C), 1.0, 6.0, ((0, 128),)),
        "mask_cot": bell_draw(key_list[1], (IMAGES, ROI_IMG, MH, MH, C), 1.0, 6.0, ((0, 128),)),
        "roi_counts": draw_roi_counts(jax.random.fold_in(key_list[10], 71), 0),
        "rpn_feats": bell_draw(key_list[3], (IMAGES, GH, GW, C), 1.0, 6.0, ((0, 128),)),
        "rpn_cot": bell_draw(key_list[4], (IMAGES, GH, GW, C), 60.0, 360.0, ((0, 128),)),
        "anchor_counts": draw_anchor_counts(jax.random.fold_in(key_list[10], 71), 0),
        "mask_weight": bell_draw(key_list[6], (9 * C, C), (9 * C) ** -0.5, 0.125, (), jnp.float32),
        "rpn_weight": bell_draw(key_list[7], (9 * C, C), (9 * C) ** -0.5, 0.125, (), jnp.float32),
        "mask_moment": bell_draw(key_list[8], (9 * C, C), 1.0, 6.0, (), jnp.float32),
        "rpn_moment": bell_draw(key_list[9], (9 * C, C), 1.0, 6.0, (), jnp.float32),
    }


def weight_grad(feats, cotan):
    grid_rows = feats.shape[1]
    grid_cols = feats.shape[2]
    chans = feats.shape[3]
    padded = jnp.pad(feats, ((0, 0), (1, 1), (1, 1), (0, 0)))
    flat_cot = cotan.reshape(-1, chans)
    blocks = []
    for row_tap in range(3):
        for col_tap in range(3):
            window = padded[:, row_tap:row_tap + grid_rows, col_tap:col_tap + grid_cols, :].reshape(-1, chans)
            blocks.append(lax.dot_general(window, flat_cot, (((0,), (0,)), ((), ())), preferred_element_type=jnp.float32))
    return jnp.concatenate(blocks, axis=0)

def reference(mask_feats, mask_cot, roi_counts, rpn_feats, rpn_cot, anchor_counts, mask_weight, rpn_weight, mask_moment, rpn_moment):
    roi_total = jnp.sum(roi_counts).astype(jnp.float32)
    anchor_total = jnp.sum(anchor_counts).astype(jnp.float32)
    slots = jnp.arange(ROI_IMG, dtype=jnp.int32)
    valid_slots = (slots[None, :] < roi_counts[:, None]).astype(jnp.bfloat16)
    masked = mask_cot * valid_slots[:, :, None, None, None]
    mask_grad = weight_grad(mask_feats.reshape(-1, MH, MH, C), masked.reshape(-1, MH, MH, C)) / roi_total
    rpn_grad = weight_grad(rpn_feats, rpn_cot) / anchor_total
    new_mask_moment = 0.9 * mask_moment + mask_grad
    new_rpn_moment = 0.9 * rpn_moment + rpn_grad
    new_mask_weight = mask_weight - 0.02 * new_mask_moment
    new_rpn_weight = rpn_weight - 0.02 * new_rpn_moment
    return (new_mask_weight, new_rpn_weight, new_mask_moment, new_rpn_moment)
```

```python
import jax
import jax.numpy as jnp
from jax import lax
from jax.experimental import pallas as pl
from jax.experimental.pallas import tpu as pltpu
from jax.sharding import PartitionSpec as P

bf16 = jnp.bfloat16
f32 = jnp.float32
RING = 4
PLANE = sorted(
    ((db, dc) for db in range(4) for dc in range(4) if (db, dc) != (0, 0)),
    key=lambda d: min(d[0], 4 - d[0]) + min(d[1], 4 - d[1]),
)
CUBE = [
    (dx, dy, dz)
    for dx in range(4)
    for dy in range(4)
    for dz in range(4)
    if 1 <= (dx != 0) + (dy != 0) + (dz != 0) <= 2
]


def kernel(
    xm_hbm, ym_hbm, roi, xr_hbm, yr_hbm, anchor, wm_hbm, wr_hbm, mm_hbm, mr_hbm,
    out_wm, out_wr, out_mm, out_mr,
    xm, ym, xr, yr, xt, grad, other, part, inbox, relay, chunk, plane_in, full,
    weights, moments, count, count_in,
    load_sem, pair_send, pair_recv, ring_send, ring_recv, plane_send, plane_recv,
    fan_send, fan_recv, ag_send, ag_recv, last_send, last_recv, count_send, count_recv,
):
    gx = lax.axis_index("gx")
    gy = lax.axis_index("gy")
    core = lax.rem(gx, 2)
    pos = (gx // 2, lax.rem(gy, 4), gy // 4)

    def at(offset, own_core=True):
        x, y, z = (lax.rem(p + d, RING) if d else p for p, d in zip(pos, offset))
        return (x * 2 + (core if own_core else 1 - core), z * 4 + y)

    def along(axis, d):
        offset = [0, 0, 0]
        offset[axis] = d % RING
        return at(offset)

    def send(src, dst, send_sem, recv_sem, device):
        copy = pltpu.make_async_remote_copy(
            src_ref=src, dst_ref=dst, send_sem=send_sem, recv_sem=recv_sem,
            device_id=device, device_id_type=pl.DeviceIdType.MESH,
        )
        copy.start()
        sent.append(copy)
        return copy

    sent = []
    partner = at((0, 0, 0), own_core=False)

    barrier = pltpu.get_barrier_semaphore()
    for device in [partner] + [at(o) for o in CUBE]:
        pl.semaphore_signal(barrier, inc=1, device_id=device, device_id_type=pl.DeviceIdType.MESH)

    loads = [
        pltpu.make_async_copy(xm_hbm, xm.at[:, :, pl.ds(1, 14)], load_sem.at[0]),
        pltpu.make_async_copy(ym_hbm, ym.at[:, pl.ds(1, 14)], load_sem.at[1]),
        pltpu.make_async_copy(xr_hbm, xr, load_sem.at[2]),
        pltpu.make_async_copy(yr_hbm.at[pl.ds(0, 1536)], yr.at[pl.ds(32, 1536)], load_sem.at[3]),
        pltpu.make_async_copy(yr_hbm.at[pl.ds(1536, 1536)], yr.at[pl.ds(1632, 1536)], load_sem.at[4]),
        pltpu.make_async_copy(mm_hbm, moments.at[0], load_sem.at[5]),
        pltpu.make_async_copy(mr_hbm, moments.at[1], load_sem.at[6]),
        pltpu.make_async_copy(wm_hbm, weights.at[0], load_sem.at[7]),
        pltpu.make_async_copy(wr_hbm, weights.at[1], load_sem.at[8]),
    ]
    for copy in loads[:5]:
        copy.start()
    for i in range(2):
        for e in (0, 15):
            xm[i, :, e] = jnp.zeros((14, 8, 256), bf16)
            ym[i, e] = jnp.zeros((14, 8, 256), bf16)
        for e in (0, 49):
            yr[pl.ds(1600 * i + 32 * e, 32), :] = jnp.zeros((32, 256), bf16)

    count[0, 0] = jnp.full((8, 128), (roi[0] + roi[1]).astype(f32))
    count[0, 1] = jnp.full((8, 128), (anchor[0] + anchor[1]).astype(f32))

    def prepare_mask():
        slot = lax.broadcasted_iota(jnp.int32, (8, 256), 0)

        def tap(b, carry):
            for i in range(2):
                keep = slot < roi[i]
                v = xm[i, :, pl.ds(b, 14)]
                v = jnp.where(keep[None, None], v, jnp.zeros_like(v))
                xt[pl.ds(pl.multiple_of(b * 256, 256), 256), i * 1568:(i + 1) * 1568] = v.reshape(1568, 256).T
            return carry

        lax.fori_loop(0, 3, tap, 0)

    def prepare_rpn():
        lane = lax.broadcasted_iota(jnp.int32, (256, 256), 1) % 32
        first = lane == 0
        last = lane == 31
        zero = jnp.zeros((256, 256), bf16)

        def piece(k, carry):
            col = pl.multiple_of(k * 256, 256)
            v = xr[pl.ds(col, 256), :].T
            xt[256:512, pl.ds(col, 256)] = v
            xt[0:256, pl.ds(col, 256)] = jnp.where(first, zero, pltpu.roll(v, 1, 1))
            xt[512:768, pl.ds(col, 256)] = jnp.where(last, zero, pltpu.roll(v, 255, 1))
            return carry

        lax.fori_loop(0, 12, piece, 0, unroll=4)

    def multiply(kind, a):
        if kind == 0:
            y = jnp.concatenate([ym[i, pl.ds(2 - a, 14)].reshape(1568, 256) for i in range(2)], 0)
            r = jnp.dot(xt[:, 0:3136], y, preferred_element_type=f32)
        else:
            y = jnp.concatenate([yr[1600 * i + 32 * (2 - a):1600 * i + 32 * (2 - a) + 1536, :] for i in range(2)], 0)
            r = jnp.dot(xt[:, 0:3072], y, preferred_element_type=f32)
        for h in range(2):
            grad[kind, a, h] = r[:, 128 * h:128 * h + 128].reshape(96, 8, 128)
        send(grad.at[kind, a, 1 - core], other.at[kind, a], pair_send.at[kind, a], pair_recv.at[kind, a], partner)

    def landed(dst, sem):
        pltpu.make_async_copy(dst, dst, sem).wait()

    def halves(kind, a):
        return part.at[kind, a], inbox.at[kind, a], ring_send.at[kind, a], ring_recv.at[kind, a], pos[a]

    def combine(kind, a):
        landed(other.at[kind, a], pair_recv.at[kind, a])
        total = grad[kind, a, core] + other[kind, a]
        s, box, ss, rs, i = halves(kind, a)
        s[...] = total.reshape(4, 24, 8, 128)
        right, left = along(a, 1), along(a, -1)
        far, nxt, prv = (lax.rem(i + d, RING) for d in (2, 1, 3))
        send(s.at[far, pl.ds(0, 12)], box.at[0], ss.at[0], rs.at[0], right)
        send(s.at[far, pl.ds(12, 12)], box.at[1], ss.at[1], rs.at[1], left)
        send(s.at[nxt, pl.ds(12, 12)], box.at[2], ss.at[2], rs.at[2], right)
        send(s.at[prv, pl.ds(0, 12)], box.at[3], ss.at[3], rs.at[3], left)

    def pass_on(kind, a):
        s, box, ss, rs, i = halves(kind, a)
        nxt, prv = lax.rem(i + 1, RING), lax.rem(i + 3, RING)
        landed(box.at[0], rs.at[0])
        relay[kind, a, 0] = s[nxt, 0:12] + box[0]
        send(relay.at[kind, a, 0], box.at[4], ss.at[4], rs.at[4], along(a, 1))
        landed(box.at[1], rs.at[1])
        relay[kind, a, 1] = s[prv, 12:24] + box[1]
        send(relay.at[kind, a, 1], box.at[5], ss.at[5], rs.at[5], along(a, -1))

    def finish(kind, a):
        s, box, ss, rs, i = halves(kind, a)
        for k in (2, 3, 4, 5):
            landed(box.at[k], rs.at[k])
        chunk[a, kind * 24:kind * 24 + 12] = s[i, 0:12] + box[3] + box[4]
        chunk[a, kind * 24 + 12:kind * 24 + 24] = s[i, 12:24] + box[2] + box[5]

    def plane(a, db, dc):
        offset = [0, 0, 0]
        offset[(a + 1) % 3] = db
        offset[(a + 2) % 3] = dc
        return at(offset)

    def place(a, db=0, dc=0):
        b, c = pos[(a + 1) % 3], pos[(a + 2) % 3]
        return lax.rem(b + db, RING) * 4 + lax.rem(c + dc, RING)

    def scatter(a):
        for k, (db, dc) in enumerate(PLANE):
            send(
                chunk.at[a, pl.ds(3 * place(a, db, dc), 3)], plane_in.at[a, k],
                plane_send.at[a, k], plane_recv.at[a, k], plane(a, db, dc),
            )

    def reduce_and_fan(a):
        p = place(a)
        total = chunk[a, pl.ds(3 * p, 3)]
        for k in range(15):
            landed(plane_in.at[a, k], plane_recv.at[a, k])
            total = total + plane_in[a, k]
        mine = full.at[core, a, pos[a], pl.ds(3 * p, 3)]
        mine[...] = total / count[4, p // 8][None]
        for k, (db, dc) in enumerate(PLANE):
            send(mine, mine, fan_send.at[a, k], fan_recv.at[a, k], plane(a, db, dc))

    def to_partner(a, j, lo, n, slot):
        piece = full.at[core, a, j, pl.ds(lo, n)]
        send(piece, piece, last_send.at[a, slot], last_recv.at[a, slot], partner)

    def gather_start(a):
        i = pos[a]
        for k, (db, dc) in enumerate(PLANE):
            p = place(a, RING - db if db else 0, RING - dc if dc else 0)
            landed(full.at[core, a, i, pl.ds(3 * p, 3)], fan_recv.at[a, k])
        right, left = along(a, 1), along(a, -1)
        lo, hi = (full.at[core, a, i, pl.ds(h, 24)] for h in (0, 24))
        send(lo, lo, ag_send.at[a, 0], ag_recv.at[a, 0], right)
        send(hi, hi, ag_send.at[a, 1], ag_recv.at[a, 1], left)
        send(hi, hi, ag_send.at[a, 2], ag_recv.at[a, 2], right)
        send(lo, lo, ag_send.at[a, 3], ag_recv.at[a, 3], left)
        to_partner(a, i, 0, 48, 0)

    def gather_pass(a):
        i = pos[a]
        nxt, prv = lax.rem(i + 1, RING), lax.rem(i + 3, RING)
        piece = full.at[core, a, prv, pl.ds(0, 24)]
        landed(piece, ag_recv.at[a, 0])
        send(piece, piece, ag_send.at[a, 4], ag_recv.at[a, 4], along(a, 1))
        to_partner(a, prv, 0, 24, 1)
        piece = full.at[core, a, nxt, pl.ds(24, 24)]
        landed(piece, ag_recv.at[a, 1])
        send(piece, piece, ag_send.at[a, 5], ag_recv.at[a, 5], along(a, -1))
        to_partner(a, nxt, 24, 24, 2)

    def gather_near(a):
        i = pos[a]
        nxt, prv = lax.rem(i + 1, RING), lax.rem(i + 3, RING)
        landed(full.at[core, a, prv, pl.ds(24, 24)], ag_recv.at[a, 2])
        to_partner(a, prv, 24, 24, 3)
        landed(full.at[core, a, nxt, pl.ds(0, 24)], ag_recv.at[a, 3])
        to_partner(a, nxt, 0, 24, 4)

    def gather_far(a):
        far = lax.rem(pos[a] + 2, RING)
        landed(full.at[core, a, far, pl.ds(0, 24)], ag_recv.at[a, 4])
        to_partner(a, far, 0, 24, 5)
        landed(full.at[core, a, far, pl.ds(24, 24)], ag_recv.at[a, 5])
        to_partner(a, far, 24, 24, 6)

    def from_partner(a, slot):
        i = pos[a]
        d, lo, n = ((0, 0, 48), (3, 0, 24), (1, 24, 24), (3, 24, 24), (1, 0, 24), (2, 0, 24), (2, 24, 24))[slot]
        landed(full.at[1 - core, a, lax.rem(i + d, RING), pl.ds(lo, n)], last_recv.at[a, slot])

    outs = ((out_wm, out_mm), (out_wr, out_mr))

    def update(a, d, kind, h):
        j = lax.rem(pos[a] + d, RING)
        g = full[h, a, j, kind * 24:kind * 24 + 24].reshape(192, 128)
        rows = pl.ds(pl.multiple_of(a * 768 + j * 192, 64), 192)
        lanes = pl.ds(pl.multiple_of(h * 128, 128), 128)
        new_w, new_m = outs[kind]
        m = 0.9 * moments[kind, rows, lanes] + g
        new_m[rows, lanes] = m
        new_w[rows, lanes] = weights[kind, rows, lanes] - 0.02 * m

    def count_pair():
        send(count.at[0], count_in.at[0], count_send.at[0], count_recv.at[0], partner)

    def count_axis(axis):
        if axis == 0:
            landed(count_in.at[0], count_recv.at[0])
            count[1] = count[0] + count_in[0]
        else:
            count_close(axis - 1)
        for d in (1, 2, 3):
            k = 3 * axis + d
            send(count.at[axis + 1], count_in.at[k], count_send.at[k], count_recv.at[k], along(axis, d))

    def count_close(axis):
        total = count[axis + 1]
        for d in (1, 2, 3):
            k = 3 * axis + d
            landed(count_in.at[k], count_recv.at[k])
            total = total + count_in[k]
        count[axis + 2] = total

    loads[0].wait()
    loads[1].wait()
    prepare_mask()
    pl.semaphore_wait(barrier, 1 + len(CUBE))
    count_pair()
    multiply(0, 0)
    count_axis(0)
    multiply(0, 1)
    combine(0, 0)
    count_axis(1)
    multiply(0, 2)
    pass_on(0, 0)
    combine(0, 1)
    count_axis(2)
    for copy in loads[2:5]:
        copy.wait()
    for copy in loads[5:]:
        copy.start()
    prepare_rpn()
    pass_on(0, 1)
    combine(0, 2)
    multiply(1, 0)
    pass_on(0, 2)
    finish(0, 0)
    multiply(1, 1)
    combine(1, 0)
    finish(0, 1)
    multiply(1, 2)
    pass_on(1, 0)
    combine(1, 1)
    finish(0, 2)
    count_close(2)
    combine(1, 2)
    pass_on(1, 1)
    finish(1, 0)
    scatter(0)
    pass_on(1, 2)
    finish(1, 1)
    scatter(1)
    finish(1, 2)
    scatter(2)
    for a in range(3):
        reduce_and_fan(a)
    for a in range(3):
        gather_start(a)
    for copy in loads[5:]:
        copy.wait()
    for a in range(3):
        gather_pass(a)
    for a in range(3):
        for kind in range(2):
            update(a, 0, kind, core)
    for a in range(3):
        gather_near(a)
    for a in range(3):
        for kind in range(2):
            update(a, 1, kind, core)
            update(a, 3, kind, core)
    for a in range(3):
        for slot in range(5):
            from_partner(a, slot)
        for kind in range(2):
            for d in (0, 1, 3):
                update(a, d, kind, 1 - core)
    for a in range(3):
        gather_far(a)
    for a in range(3):
        for kind in range(2):
            update(a, 2, kind, core)
    for a in range(3):
        for slot in (5, 6):
            from_partner(a, slot)
        for kind in range(2):
            update(a, 2, kind, 1 - core)
    for copy in sent:
        copy.wait_send()


def on_device(xm, ym, roi, xr, yr, anchor, wm, wr, mm, mr):
    images, slots, side, _, chans = xm.shape
    vmem = pltpu.VMEM
    dma = pltpu.SemaphoreType.DMA
    anywhere = pl.BlockSpec(memory_space=pl.ANY)
    smem = pl.BlockSpec(memory_space=pltpu.SMEM)
    shape = jax.ShapeDtypeStruct(wm.shape, f32)
    xm = xm.transpose(0, 2, 3, 1, 4)
    ym = ym.transpose(0, 2, 3, 1, 4)
    return pl.pallas_call(
        kernel,
        out_shape=(shape,) * 4,
        in_specs=[anywhere, anywhere, smem, anywhere, anywhere, smem] + [anywhere] * 4,
        out_specs=(pl.BlockSpec(memory_space=vmem),) * 4,
        scratch_shapes=[
            vmem((2, 14, 16, 8, 256), bf16),
            vmem((2, 16, 14, 8, 256), bf16),
            vmem((3072, 256), bf16),
            vmem((3200, 256), bf16),
            vmem((768, 3200), bf16),
            vmem((2, 3, 2, 96, 8, 128), f32),
            vmem((2, 3, 96, 8, 128), f32),
            vmem((2, 3, 4, 24, 8, 128), f32),
            vmem((2, 3, 6, 12, 8, 128), f32),
            vmem((2, 3, 2, 12, 8, 128), f32),
            vmem((3, 48, 8, 128), f32),
            vmem((3, 15, 3, 8, 128), f32),
            vmem((2, 3, 4, 48, 8, 128), f32),
            vmem((2, 2304, 256), f32),
            vmem((2, 2304, 256), f32),
            vmem((5, 2, 8, 128), f32),
            vmem((10, 2, 8, 128), f32),
            dma((9,)),
            dma((2, 3)), dma((2, 3)),
            dma((2, 3, 6)), dma((2, 3, 6)),
            dma((3, 15)), dma((3, 15)),
            dma((3, 15)), dma((3, 15)),
            dma((3, 6)), dma((3, 6)),
            dma((3, 7)), dma((3, 7)),
            dma((10,)), dma((10,)),
        ],
        compiler_params=pltpu.CompilerParams(
            collective_id=0, has_side_effects=True, vmem_limit_bytes=62 << 20
        ),
    )(xm, ym, roi, xr.reshape(-1, chans), yr.reshape(-1, chans), anchor, wm, wr, mm, mr)


def solution(mesh):
    images = ("gx", "gy")
    placed = (
        P(images, None, None, None, None),
        P(images, None, None, None, None),
        P(images),
        P(images, None, None, None),
        P(images, None, None, None),
        P(images),
        P(), P(), P(), P(),
    )
    return jax.shard_map(
        on_device, mesh=mesh, in_specs=placed, out_specs=(P(), P(), P(), P()), check_vma=False
    )
```

```python
import jax
import jax.numpy as jnp
from jax import lax
from jax.experimental import pallas as pl
from jax.experimental.pallas import tpu as pltpu
from jax.sharding import PartitionSpec as P

bf16 = jnp.bfloat16
f32 = jnp.float32
RING = 4
AWAY = (1, 3, 2)
PLANE = sorted(
    ((db, dc) for db in range(4) for dc in range(4) if (db, dc) != (0, 0)),
    key=lambda d: min(d[0], 4 - d[0]) + min(d[1], 4 - d[1]),
)
CUBE = [
    (dx, dy, dz)
    for dx in range(4)
    for dy in range(4)
    for dz in range(4)
    if 1 <= (dx != 0) + (dy != 0) + (dz != 0) <= 2
]
JOBS = tuple((kind, a) for kind in range(2) for a in range(3))


def kernel(
    xm_hbm, ym_hbm, roi, xr_hbm, yr_hbm, anchor, wm_hbm, wr_hbm, mm_hbm, mr_hbm,
    out_wm, out_wr, out_mm, out_mr,
    xm, ym, xr, yr, xt, grad, other, part, inbox, line, plane_in, full,
    weights, moments, count, count_in,
    load_sem, pair_send, pair_recv, one_send, one_recv, plane_send, plane_recv, fan_send, fan_recv,
    back1_send, back1_recv, last_send, last_recv,
    count_send, count_recv,
):
    gx = lax.axis_index("gx")
    gy = lax.axis_index("gy")
    core = lax.rem(gx, 2)
    pos = (gx // 2, lax.rem(gy, 4), gy // 4)

    def at(offset, own_core=True):
        x, y, z = (lax.rem(p + d, RING) if d else p for p, d in zip(pos, offset))
        return (x * 2 + (core if own_core else 1 - core), z * 4 + y)

    def along(axis, d):
        offset = [0, 0, 0]
        offset[axis] = d % RING
        return at(offset)

    def start(src, dst, send_sem, recv_sem, device):
        copy = pltpu.make_async_remote_copy(
            src_ref=src, dst_ref=dst, send_sem=send_sem, recv_sem=recv_sem,
            device_id=device, device_id_type=pl.DeviceIdType.MESH,
        )
        copy.start()
        return copy

    def send(*args):
        sent.append(start(*args))

    sent = []
    partner = at((0, 0, 0), own_core=False)

    loads = [
        pltpu.make_async_copy(xm_hbm, xm.at[:, :, pl.ds(1, 14)], load_sem.at[0]),
        pltpu.make_async_copy(ym_hbm, ym.at[:, pl.ds(1, 14)], load_sem.at[1]),
        pltpu.make_async_copy(xr_hbm, xr, load_sem.at[2]),
        pltpu.make_async_copy(yr_hbm.at[pl.ds(0, 1536)], yr.at[pl.ds(32, 1536)], load_sem.at[3]),
        pltpu.make_async_copy(yr_hbm.at[pl.ds(1536, 1536)], yr.at[pl.ds(1632, 1536)], load_sem.at[4]),
        pltpu.make_async_copy(mm_hbm, moments.at[0], load_sem.at[5]),
        pltpu.make_async_copy(mr_hbm, moments.at[1], load_sem.at[6]),
        pltpu.make_async_copy(wm_hbm, weights.at[0], load_sem.at[7]),
        pltpu.make_async_copy(wr_hbm, weights.at[1], load_sem.at[8]),
    ]
    for copy in loads[:2]:
        copy.start()
    barrier = pltpu.get_barrier_semaphore()
    for device in [partner] + [at(o) for o in CUBE]:
        pl.semaphore_signal(barrier, inc=1, device_id=device, device_id_type=pl.DeviceIdType.MESH)
    for i in range(2):
        for e in (0, 15):
            xm[i, :, e] = jnp.zeros((14, 8, 256), bf16)
            ym[i, e] = jnp.zeros((14, 8, 256), bf16)
        for e in (0, 49):
            yr[pl.ds(1600 * i + 32 * e, 32), :] = jnp.zeros((32, 256), bf16)

    count[0, 0] = jnp.full((8, 128), (roi[0] + roi[1]).astype(f32))
    count[0, 1] = jnp.full((8, 128), (anchor[0] + anchor[1]).astype(f32))

    def prepare_mask():
        slot = lax.broadcasted_iota(jnp.int32, (8, 256), 0)

        def tap(b, carry):
            for i in range(2):
                keep = slot < roi[i]
                v = xm[i, :, pl.ds(b, 14)]
                v = jnp.where(keep[None, None], v, jnp.zeros_like(v))
                xt[pl.ds(pl.multiple_of(b * 256, 256), 256), i * 1568:(i + 1) * 1568] = v.reshape(1568, 256).T
            return carry

        lax.fori_loop(0, 3, tap, 0)

    def prepare_rpn():
        lane = lax.broadcasted_iota(jnp.int32, (256, 256), 1) % 32
        first = lane == 0
        last = lane == 31
        zero = jnp.zeros((256, 256), bf16)

        def piece(k, carry):
            col = pl.multiple_of(k * 256, 256)
            v = xr[pl.ds(col, 256), :].T
            xt[256:512, pl.ds(col, 256)] = v
            xt[0:256, pl.ds(col, 256)] = jnp.where(first, zero, pltpu.roll(v, 1, 1))
            xt[512:768, pl.ds(col, 256)] = jnp.where(last, zero, pltpu.roll(v, 255, 1))
            return carry

        lax.fori_loop(0, 12, piece, 0, unroll=4)

    def multiply(kind, a):
        if kind == 0:
            y = jnp.concatenate([ym[i, pl.ds(2 - a, 14)].reshape(1568, 256) for i in range(2)], 0)
        else:
            y = jnp.concatenate([yr[1600 * i + 32 * (2 - a):1600 * i + 32 * (2 - a) + 1536, :] for i in range(2)], 0)
        for m in range(2):
            r = jnp.dot(xt[384 * m:384 * m + 384, 0:y.shape[0]], y, preferred_element_type=f32)
            for h in range(2):
                grad[kind, a, h, 48 * m:48 * m + 48] = r[:, 128 * h:128 * h + 128].reshape(48, 8, 128)

    def exchange(kind, a):
        send(grad.at[kind, a, 1 - core], other.at[kind, a], pair_send.at[kind, a], pair_recv.at[kind, a], partner)

    def landed(dst, sem):
        pltpu.make_async_copy(dst, dst, sem).wait()

    def combine(job):
        kind, a = JOBS[job]
        landed(other.at[kind, a], pair_recv.at[kind, a])
        total = grad[kind, a, core] + other[kind, a]
        part[job] = total.reshape(3, RING, 8, 8, 128)
        for c in range(3):
            for slot, d in enumerate(AWAY):
                send(
                    part.at[job, c, lax.rem(pos[c] + d, RING)], inbox.at[job, c, slot],
                    one_send.at[job, c, slot], one_recv.at[job, c, slot], along(c, d),
                )

    def first(job):
        for c in range(3):
            total = part[job, c, pos[c]]
            for slot in range(3):
                landed(inbox.at[job, c, slot], one_recv.at[job, c, slot])
                total = total + inbox[job, c, slot]
            line[c, 8 * job:8 * job + 8] = total

    def plane(c, db, dc):
        offset = [0, 0, 0]
        offset[(c + 1) % 3] = db
        offset[(c + 2) % 3] = dc
        return at(offset)

    def place(c, db=0, dc=0):
        b, k = pos[(c + 1) % 3], pos[(c + 2) % 3]
        return pl.ds(12 * lax.rem(b + db, RING) + 3 * lax.rem(k + dc, RING), 3)

    def scatter(c):
        for k, (db, dc) in enumerate(PLANE):
            send(
                line.at[c, place(c, db, dc)], plane_in.at[c, k],
                plane_send.at[c, k], plane_recv.at[c, k], plane(c, db, dc),
            )

    def fan(c):
        total = line[c, place(c)]
        for k in range(15):
            landed(plane_in.at[c, k], plane_recv.at[c, k])
            total = total + plane_in[c, k]
        mine = full.at[core, c, pos[c], place(c)]
        mine[...] = total / count[4, pos[(c + 1) % 3] // 2][None]
        for k, (db, dc) in enumerate(PLANE):
            send(mine, mine, fan_send.at[c, k], fan_recv.at[c, k], plane(c, db, dc))

    def gathered(c, d, h):
        return full.at[h, c, lax.rem(pos[c] + d, RING)]

    def half(c, d, h):
        return full.at[core, c, lax.rem(pos[c] + d, RING), pl.ds(24 * h, 24)]

    def share(c, d, h, slot, step):
        piece = half(c, d, h)
        send(piece, piece, back1_send.at[c, slot], back1_recv.at[c, slot], along(c, step))

    def to_partner(c, d):
        piece = gathered(c, d, core)
        send(piece, piece, last_send.at[c, d], last_recv.at[c, d], partner)

    def back1(c):
        for k, (db, dc) in enumerate(PLANE):
            landed(full.at[core, c, pos[c], place(c, (4 - db) % 4, (4 - dc) % 4)], fan_recv.at[c, k])
        share(c, 0, 0, 0, 1)
        share(c, 0, 1, 1, 3)
        share(c, 0, 1, 2, 1)
        share(c, 0, 0, 3, 3)
        to_partner(c, 0)

    def relay(c):
        landed(half(c, 3, 0), back1_recv.at[c, 0])
        share(c, 3, 0, 4, 1)
        landed(half(c, 1, 1), back1_recv.at[c, 1])
        share(c, 1, 1, 5, 3)

    def near(c):
        landed(half(c, 3, 1), back1_recv.at[c, 2])
        to_partner(c, 3)
        landed(half(c, 1, 0), back1_recv.at[c, 3])
        to_partner(c, 1)

    def far(c):
        landed(half(c, 2, 0), back1_recv.at[c, 4])
        landed(half(c, 2, 1), back1_recv.at[c, 5])
        to_partner(c, 2)

    outs = ((out_wm, out_mm), (out_wr, out_mr))

    def update(c, d, h):
        j = lax.rem(pos[c] + d, RING)
        lanes = pl.ds(pl.multiple_of(h * 128, 128), 128)
        for job, (kind, a) in enumerate(JOBS):
            g = full[h, c, j, 8 * job:8 * job + 8].reshape(64, 128)
            rows = pl.ds(pl.multiple_of(a * 768 + c * 256 + j * 64, 64), 64)
            new_w, new_m = outs[kind]
            m = 0.9 * moments[kind, rows, lanes] + g
            new_m[rows, lanes] = m
            new_w[rows, lanes] = weights[kind, rows, lanes] - 0.02 * m

    def own(c, d):
        update(c, d, core)

    def theirs(c, d):
        landed(gathered(c, d, 1 - core), last_recv.at[c, d])
        update(c, d, 1 - core)

    def count_pair():
        send(count.at[0], count_in.at[0], count_send.at[0], count_recv.at[0], partner)

    def count_axis(axis):
        if axis == 0:
            landed(count_in.at[0], count_recv.at[0])
            count[1] = count[0] + count_in[0]
        else:
            count_close(axis - 1)
        for d in (1, 2, 3):
            k = 3 * axis + d
            send(count.at[axis + 1], count_in.at[k], count_send.at[k], count_recv.at[k], along(axis, d))

    def count_close(axis):
        total = count[axis + 1]
        for d in (1, 2, 3):
            k = 3 * axis + d
            landed(count_in.at[k], count_recv.at[k])
            total = total + count_in[k]
        count[axis + 2] = total

    def later_loads():
        for copy in loads[2:5]:
            copy.wait()
        for copy in loads[5:]:
            copy.start()

    def weights_in():
        for copy in loads[5:]:
            copy.wait()

    def enter():
        pl.semaphore_wait(barrier, 1 + len(CUBE))

    steps = [
        (multiply, 0, 0,),
        (enter,),
        (exchange, 0, 0,),
        (count_pair,),
        (multiply, 0, 1,),
        (exchange, 0, 1,),
        (count_axis, 0,),
        (combine, 0,),
        (multiply, 0, 2,),
        (exchange, 0, 2,),
        (combine, 1,),
        (later_loads,),
        (prepare_rpn,),
        (count_axis, 1,),
        (combine, 2,),
        (multiply, 1, 0,),
        (exchange, 1, 0,),
        (multiply, 1, 1,),
        (exchange, 1, 1,),
        (first, 0,),
        (combine, 3,),
        (multiply, 1, 2,),
        (exchange, 1, 2,),
        (combine, 4,),
        (count_axis, 2,),
        (first, 1,),
        (first, 2,),
        (combine, 5,),
        (first, 3,),
        (count_close, 2,),
        (first, 4,),
        (first, 5,),
        (scatter, 0,),
        (scatter, 1,),
        (scatter, 2,),
        (fan, 0,),
        (fan, 1,),
        (fan, 2,),
        (back1, 0,),
        (back1, 1,),
        (back1, 2,),
        (weights_in,),
        (own, 0, 0,),
        (own, 1, 0,),
        (own, 2, 0,),
        (relay, 0,),
        (relay, 1,),
        (relay, 2,),
        (theirs, 0, 0,),
        (theirs, 1, 0,),
        (theirs, 2, 0,),
        (near, 0,),
        (near, 1,),
        (near, 2,),
        (own, 0, 3,),
        (own, 0, 1,),
        (own, 1, 3,),
        (own, 1, 1,),
        (own, 2, 3,),
        (own, 2, 1,),
        (theirs, 0, 3,),
        (theirs, 0, 1,),
        (theirs, 1, 3,),
        (theirs, 1, 1,),
        (theirs, 2, 3,),
        (theirs, 2, 1,),
        (far, 0,),
        (far, 1,),
        (far, 2,),
        (own, 0, 2,),
        (own, 1, 2,),
        (own, 2, 2,),
        (theirs, 0, 2,),
        (theirs, 1, 2,),
        (theirs, 2, 2,),
    ]
    loads[0].wait()
    loads[1].wait()
    for copy in loads[2:5]:
        copy.start()
    prepare_mask()
    for step, *args in steps:
        step(*args)
    for copy in sent:
        copy.wait_send()


def write_out(*refs):
    sem = refs[8]
    rows = refs[0].shape[0] // 2
    copies = [
        pltpu.make_async_copy(refs[k].at[pl.ds(h * rows, rows)], refs[4 + k].at[pl.ds(h * rows, rows)], sem.at[2 * k + h])
        for k in range(4) for h in range(2)
    ]
    for copy in copies:
        copy.start()
    for copy in copies:
        copy.wait()


def on_device(xm, ym, roi, xr, yr, anchor, wm, wr, mm, mr):
    images, slots, side, _, chans = xm.shape
    vmem = pltpu.VMEM
    dma = pltpu.SemaphoreType.DMA
    anywhere = pl.BlockSpec(memory_space=pl.ANY)
    smem = pl.BlockSpec(memory_space=pltpu.SMEM)
    shape = jax.ShapeDtypeStruct(wm.shape, f32)
    xm = xm.transpose(0, 2, 3, 1, 4)
    ym = ym.transpose(0, 2, 3, 1, 4)
    results = pl.pallas_call(
        kernel,
        out_shape=(vmem(wm.shape, f32),) * 4,
        in_specs=[anywhere, anywhere, smem, anywhere, anywhere, smem] + [anywhere] * 4,
        out_specs=(pl.BlockSpec(memory_space=vmem),) * 4,
        scratch_shapes=[
            vmem((2, 14, 16, 8, 256), bf16),
            vmem((2, 16, 14, 8, 256), bf16),
            vmem((3072, 256), bf16),
            vmem((3200, 256), bf16),
            vmem((768, 3200), bf16),
            vmem((2, 3, 2, 96, 8, 128), f32),
            vmem((2, 3, 96, 8, 128), f32),
            vmem((6, 3, RING, 8, 8, 128), f32),
            vmem((6, 3, 3, 8, 8, 128), f32),
            vmem((3, 48, 8, 128), f32),
            vmem((3, 15, 3, 8, 128), f32),
            vmem((2, 3, RING, 48, 8, 128), f32),
            vmem((2, 2304, 256), f32),
            vmem((2, 2304, 256), f32),
            vmem((5, 2, 8, 128), f32),
            vmem((10, 2, 8, 128), f32),
            dma((9,)),
            dma((2, 3)), dma((2, 3)),
            dma((6, 3, 3)), dma((6, 3, 3)),
            dma((3, 15)), dma((3, 15)),
            dma((3, 15)), dma((3, 15)),
            dma((3, 6)), dma((3, 6)),
            dma((3, RING)), dma((3, RING)),
            dma((10,)), dma((10,)),
        ],
        compiler_params=pltpu.CompilerParams(
            collective_id=0, has_side_effects=True, vmem_limit_bytes=57606144
        ),
    )(xm, ym, roi, xr.reshape(-1, chans), yr.reshape(-1, chans), anchor, wm, wr, mm, mr)
    return pl.pallas_call(
        write_out,
        out_shape=(shape,) * 4,
        in_specs=[pl.BlockSpec(memory_space=vmem)] * 4,
        out_specs=(anywhere,) * 4,
        scratch_shapes=[dma((8,))],
        compiler_params=pltpu.CompilerParams(vmem_limit_bytes=1 << 20),
    )(*results)


def solution(mesh):
    images = ("gx", "gy")
    placed = (
        P(images, None, None, None, None),
        P(images, None, None, None, None),
        P(images),
        P(images, None, None, None),
        P(images, None, None, None),
        P(images),
        P(), P(), P(), P(),
    )
    return jax.shard_map(
        on_device, mesh=mesh, in_specs=placed, out_specs=(P(), P(), P(), P()), check_vma=False
    )
```
